256 devices in a mesh: win: 4 (over x_hi, core), sta: 64 (over y, z, x_lo).
Axes of the slice: x: 4 (x_hi: 2, x_lo: 2; x = x_hi * 2 + x_lo), y: 4, z: 8, core: 2. Of those that a mesh axis runs over, the one named last changes fastest.
Arguments:
- samples: bfloat16 [256, 2097152], P('sta', 'win'), may hold values from -6 to 6
- coarse_taps: bfloat16 [16, 512], replicated, may hold values from -0.0625 to 0.0625
- fine_taps: bfloat16 [8, 64], replicated, may hold values from -0.25 to 0.25
Outputs:
- visibilities: bfloat16 [128, 64, 2, 256, 256], P('win', 'sta')
The draws below stay inside these ranges and needn't reach their ends.
All inputs are finite; a program needn't handle non-finite values.
Results may differ from the reference program's by a relative error of at most 0.008.
Values may be sent and summed in bfloat16 or wider, within the bound.
A program may use at most 64 MiB of HBM per device.

```python
import math
import jax
import jax.numpy as jnp
from jax import lax

SIG = 256
FRAME = 512
KEEP = 128
FIRST = 64
TAPS = 16
FINE = 64
FTAPS = 8
NT = 2097152


def block_levels(rng, shape, cuts, smallest, high):
    def one(dim, shards_of):
        heights = jax.random.uniform(jax.random.fold_in(jax.random.fold_in(rng, 6), dim), (shards_of,), jnp.float32, smallest / len(cuts), high / len(cuts))
        return jnp.repeat(jnp.exp(heights), shape[dim] // shards_of).reshape((-1,) + (1,) * (len(shape) - dim - 1))

    gain = one(*cuts[0])
    for cut in cuts[1:]:
        gain = gain * one(*cut)
    return gain


def noise(key, dims, width, limit, pieces=(), kind=jnp.bfloat16):
    factor_of = block_levels(key, dims, pieces, -0.22, 0.18) if pieces else 1.0
    drawn = jax.random.normal(key, dims, jnp.float32) * width * factor_of
    return jnp.minimum(jnp.maximum(drawn, -limit), limit).astype(kind)


def setup_inputs(seed: int = 0) -> dict:
    keys = jax.random.split(jax.random.key(seed), 4)
    samples = noise(keys[0], (SIG, NT), 1.0, 6.0, ((0, 64), (1, 4)))
    coarse_taps = noise(keys[1], (TAPS, FRAME), (TAPS * FRAME) ** -0.5, 0.0625)
    fine_taps = noise(keys[2], (FTAPS, FINE), (FTAPS * FINE) ** -0.5, 0.25)
    return dict(samples=samples, coarse_taps=coarse_taps, fine_taps=fine_taps)


def coarse_matrix():
    channels = FIRST + jnp.arange(KEEP, dtype=jnp.int32)
    products = jnp.arange(FRAME, dtype=jnp.int32)[:, None] * channels[None, :]
    angles = (products % FRAME).astype(jnp.float32) * (2.0 * math.pi / FRAME)
    return jnp.concatenate([jnp.cos(angles), -jnp.sin(angles)], axis=1).astype(jnp.bfloat16)


def fine_tables():
    products = jnp.arange(FINE, dtype=jnp.int32)[:, None] * jnp.arange(FINE, dtype=jnp.int32)[None, :]
    angles = (products % FINE).astype(jnp.float32) * (2.0 * math.pi / FINE)
    return jnp.cos(angles), jnp.sin(angles)


def channelise(signal, coarse_taps, fine_taps, coarse_dft, cosines, sines):
    frame_count = NT // FRAME
    frames_all = signal.reshape(frame_count, FRAME)
    padded = jnp.concatenate([jnp.zeros((TAPS - 1, FRAME), jnp.bfloat16), frames_all], axis=0)
    windowed = jnp.zeros((frame_count, FRAME), jnp.float32)
    for tap_index in range(TAPS):
        start = TAPS - 1 - tap_index
        windowed = windowed + coarse_taps[tap_index].astype(jnp.float32)[None, :] * padded[start:start + frame_count].astype(jnp.float32)
    spectra = jnp.dot(windowed.astype(jnp.bfloat16), coarse_dft, preferred_element_type=jnp.float32).astype(jnp.bfloat16)
    history = (FTAPS - 1) * FINE
    extended = jnp.concatenate([jnp.zeros((history, 2 * KEEP), jnp.bfloat16), spectra], axis=0)
    fine_count = frame_count // FINE
    groups = extended.reshape(fine_count + FTAPS - 1, FINE, 2, KEEP)
    filtered = jnp.zeros((fine_count, FINE, 2, KEEP), jnp.float32)
    for tap_index in range(FTAPS):
        start = FTAPS - 1 - tap_index
        filtered = filtered + fine_taps[tap_index].astype(jnp.float32)[None, :, None, None] * groups[start:start + fine_count].astype(jnp.float32)
    real_part = filtered[:, :, 0]
    imag_part = filtered[:, :, 1]
    highest = lax.Precision.HIGHEST
    out_real = jnp.einsum("qj,gjk->kqg", cosines, real_part, precision=highest) + jnp.einsum("qj,gjk->kqg", sines, imag_part, precision=highest)
    out_imag = jnp.einsum("qj,gjk->kqg", cosines, imag_part, precision=highest) - jnp.einsum("qj,gjk->kqg", sines, real_part, precision=highest)
    return jnp.stack([out_real, out_imag], axis=2).astype(jnp.bfloat16)


def reference(samples, coarse_taps, fine_taps):
    coarse_dft = coarse_matrix()
    cosines, sines = fine_tables()
    spectra_all = lax.map(lambda signal: channelise(signal, coarse_taps, fine_taps, coarse_dft, cosines, sines), samples)
    frame_total = NT // (FRAME * FINE)
    highest = lax.Precision.HIGHEST

    def correlate(channel):
        channel_block = lax.dynamic_index_in_dim(spectra_all, channel, 1, keepdims=False).astype(jnp.float32)
        channel_block = jnp.transpose(channel_block, (1, 0, 2, 3))
        columns_all = channel_block.reshape(FINE, SIG, 2 * frame_total)
        turned = jnp.concatenate([channel_block[:, :, 1], -channel_block[:, :, 0]], axis=2)
        real_vis = jnp.einsum("qsc,qtc->qst", columns_all, columns_all, precision=highest)
        imag_vis = jnp.einsum("qsc,qtc->qst", turned, columns_all, precision=highest)
        return (jnp.stack([real_vis, imag_vis], axis=1) / frame_total).astype(jnp.bfloat16)

    return lax.map(correlate, jnp.arange(KEEP, dtype=jnp.int32))
```

```python
import math

import jax
import jax.numpy as jnp
from jax import lax
from jax.experimental import pallas as pl
from jax.experimental.pallas import tpu as pltpu
from jax.sharding import PartitionSpec as P

KEEP = 128
MESH_ID = pl.DeviceIdType.MESH


def from_behind(x, axis, by):
    size = lax.axis_size(axis)
    pairs = [(i, i + by) for i in range(size) if 0 <= i + by < size]
    return lax.ppermute(x, axis, pairs)


def coarse_matrix(frame_len, band_count):
    channels = frame_len // 8 + jnp.arange(band_count, dtype=jnp.int32)
    products = jnp.arange(frame_len, dtype=jnp.int32)[:, None] * channels[None, :]
    angles = (products % frame_len).astype(jnp.float32) * (2.0 * math.pi / frame_len)
    return jnp.concatenate([jnp.cos(angles), -jnp.sin(angles)], axis=1).astype(jnp.bfloat16)


def fine_tables(fine_len):
    products = (
        jnp.arange(fine_len, dtype=jnp.int32)[:, None]
        * jnp.arange(fine_len, dtype=jnp.int32)[None, :]
    )
    angles = (products % fine_len).astype(jnp.float32) * (2.0 * math.pi / fine_len)
    return (jnp.cos(angles), jnp.sin(angles))


def exchange_kernel(n_win, n_sta, send_ref, recv_ref, local_sem, send_sem, recv_sem):
    n_all = n_win * n_sta
    my_win = lax.axis_index("win")
    my_sta = lax.axis_index("sta")
    me = my_win * n_sta + my_sta
    barrier = pltpu.get_barrier_semaphore()

    def peer(step):
        other = lax.rem(me + step, n_all)
        return other, (other // n_sta, lax.rem(other, n_sta))

    def greet(step, carry):
        _, where = peer(step)
        pl.semaphore_signal(barrier, inc=1, device_id=where, device_id_type=MESH_ID)
        return carry

    lax.fori_loop(1, n_all, greet, 0)
    own = pltpu.make_async_copy(send_ref.at[me], recv_ref.at[me], local_sem)
    own.start()
    pl.semaphore_wait(barrier, n_all - 1)

    def post(step, carry):
        other, where = peer(step)
        pltpu.make_async_remote_copy(
            src_ref=send_ref.at[other],
            dst_ref=recv_ref.at[me],
            send_sem=send_sem,
            recv_sem=recv_sem,
            device_id=where,
            device_id_type=MESH_ID,
        ).start()
        return carry

    lax.fori_loop(1, n_all, post, 0)
    own.wait()
    most = recv_ref.at[pl.ds(0, n_all - 1)]
    pltpu.make_async_copy(most, most, recv_sem).wait()
    pltpu.make_async_copy(most, most, send_sem).wait()


def exchange(blocks):
    n_win, n_sta = lax.axis_size("win"), lax.axis_size("sta")

    def kernel(*refs):
        exchange_kernel(n_win, n_sta, *refs)

    return pl.pallas_call(
        kernel,
        out_shape=jax.ShapeDtypeStruct(blocks.shape, blocks.dtype),
        in_specs=[pl.BlockSpec(memory_space=pltpu.VMEM)],
        out_specs=pl.BlockSpec(memory_space=pltpu.VMEM),
        scratch_shapes=[pltpu.SemaphoreType.DMA] * 3,
        compiler_params=pltpu.CompilerParams(collective_id=0, has_side_effects=True),
        name="exchange",
    )(blocks)


def correlate(spectra_in, pieces):
    band_local, sig_count, columns = spectra_in.shape
    split_view = spectra_in.reshape(band_local, sig_count, pieces, 2, columns // (2 * pieces))
    turned = jnp.stack([split_view[:, :, :, 1], -split_view[:, :, :, 0]], axis=3).reshape(
        band_local, sig_count, columns
    )
    real_vis = jnp.einsum("ksc,ktc->kst", spectra_in, spectra_in, preferred_element_type=jnp.float32)
    imag_vis = jnp.einsum("ksc,ktc->kst", turned, spectra_in, preferred_element_type=jnp.float32)
    return jnp.stack([real_vis, imag_vis], axis=1)[:, None]


def per_device(samples, coarse_taps, fine_taps):
    sig_local, samp_local = samples.shape
    tap_count, frame_len = coarse_taps.shape
    fine_tap_count, fine_len = fine_taps.shape
    band_count = KEEP
    n_win, n_sta = lax.axis_size("win"), lax.axis_size("sta")
    frame_count = samp_local // frame_len
    frames_local = samples.reshape(sig_local, frame_count, frame_len)
    earlier = from_behind(frames_local[:, frame_count - (tap_count - 1) :], "win", 1)
    padded = jnp.concatenate([earlier, frames_local], axis=1)
    windowed = jnp.zeros((sig_local, frame_count, frame_len), jnp.float32)
    for tap_index in range(tap_count):
        start = tap_count - 1 - tap_index
        windowed = windowed + coarse_taps[tap_index].astype(jnp.float32)[None, None, :] * padded[
            :, start : start + frame_count
        ].astype(jnp.float32)
    spectra = jnp.dot(
        windowed.astype(jnp.bfloat16).reshape(sig_local * frame_count, frame_len),
        coarse_matrix(frame_len, band_count),
        preferred_element_type=jnp.float32,
    )
    spectra = spectra.astype(jnp.bfloat16).reshape(sig_local, frame_count, 2 * band_count)
    history = (fine_tap_count - 1) * fine_len
    carried = from_behind(spectra[:, frame_count - history :], "win", 1)
    extended = jnp.concatenate([carried, spectra], axis=1)
    fine_count = frame_count // fine_len
    groups = extended.reshape(sig_local, fine_count + fine_tap_count - 1, fine_len, 2, band_count)
    filtered = jnp.zeros((sig_local, fine_count, fine_len, 2, band_count), jnp.float32)
    for tap_index in range(fine_tap_count):
        start = fine_tap_count - 1 - tap_index
        filtered = filtered + fine_taps[tap_index].astype(jnp.float32)[
            None, None, :, None, None
        ] * groups[:, start : start + fine_count].astype(jnp.float32)
    cosines, sines = fine_tables(fine_len)
    real_part = filtered[:, :, :, 0]
    imag_part = filtered[:, :, :, 1]
    highest = lax.Precision.HIGHEST
    out_real = jnp.einsum("qj,sgjk->kqsg", cosines, real_part, precision=highest) + jnp.einsum(
        "qj,sgjk->kqsg", sines, imag_part, precision=highest
    )
    out_imag = jnp.einsum("qj,sgjk->kqsg", cosines, imag_part, precision=highest) - jnp.einsum(
        "qj,sgjk->kqsg", sines, real_part, precision=highest
    )
    band_local = band_count // n_win
    block_lanes = sig_local * 2 * fine_count
    local_spectra = (
        jnp.stack([out_real, out_imag], axis=3)
        .astype(jnp.bfloat16)
        .reshape(n_win, band_local, n_sta, block_lanes)
    )
    blocks = jnp.transpose(local_spectra, (0, 2, 1, 3)).reshape(n_win * n_sta, band_local, block_lanes)
    moved = exchange(blocks).reshape(n_win, n_sta, band_local, sig_local, 2 * fine_count)
    moved = jnp.transpose(moved, (2, 1, 3, 0, 4)).reshape(
        band_local, n_sta * sig_local, n_win * 2 * fine_count
    )
    frame_total = fine_count * n_win
    return (correlate(moved, n_win) / frame_total).astype(jnp.bfloat16)


def solution(mesh):
    placed = (P("sta", "win"), P(), P())
    return jax.shard_map(
        per_device,
        mesh=mesh,
        in_specs=placed,
        out_specs=P("win", "sta", None, None, None),
        check_vma=False,
    )
```

```python
import math

import jax
import jax.numpy as jnp
import numpy as np
from jax import lax
from jax.experimental import pallas as pl
from jax.experimental.pallas import tpu as pltpu
from jax.sharding import PartitionSpec as P

KEEP = 128
QUAD = 4
MESH_ID = pl.DeviceIdType.MESH
NT_DIMS = (((1,), (1,)), ((), ()))


def coarse_matrix(frame_len, band_count):
    channels = frame_len // 8 + np.arange(band_count)
    angles = (np.arange(frame_len)[:, None] * channels[None, :]) % frame_len
    angles = angles.astype(np.float32) * np.float32(2.0 * math.pi / frame_len)
    return np.concatenate([np.cos(angles), -np.sin(angles)], axis=1).astype(jnp.bfloat16)


def fine_matrix(fine_len):
    angles = (np.arange(fine_len)[:, None] * np.arange(fine_len)[None, :]) % fine_len
    angles = angles.astype(np.float32) * np.float32(2.0 * math.pi / fine_len)
    cosines, sines = np.cos(angles), np.sin(angles)
    real_rows = np.concatenate([cosines, sines], axis=1)
    imag_rows = np.concatenate([-sines, cosines], axis=1)
    both = np.stack([real_rows, imag_rows], axis=1)
    return np.repeat(both.reshape(2 * fine_len, 2 * fine_len), QUAD, axis=0).astype(np.float32)


def pick_matrix(channels, senders, lanes):
    row = np.arange(channels * senders)
    col = np.arange(senders * lanes)
    same_sender = (row % senders)[:, None] == (col // lanes)[None, :]
    same_channel = (row // senders)[:, None] == (col % channels)[None, :]
    return (same_sender & same_channel).astype(jnp.bfloat16)


def make_channeliser(n_win, n_sta, sig_count, frame_count, tap_count, frame_len, fine_tap_count, fine_len):
    n_all = n_win * n_sta
    cols = frame_len // 128
    halo_rows = 16
    block = 128
    n_blocks = frame_count // block
    fine_count = frame_count // fine_len
    frame_rows = 2 * fine_len
    old_rows = (fine_tap_count - 1) * frame_rows
    span = fine_tap_count - 1 + QUAD
    n_quads = fine_count // QUAD
    band_local = KEEP // n_win
    group = 8
    n_groups = n_sta // group

    def kernel(
        x_ref, coarse_ref, fine_ref, dft_ref, table_ref, pick_ref, out_ref,
        wide, edge, spec, banded, stage, outbox, inbox,
        own_sem, edge_send, edge_recv, old_send, old_recv, send_sem, recv_sem,
    ):
        my_win = lax.axis_index("win")
        my_sta = lax.axis_index("sta")
        barrier = pltpu.get_barrier_semaphore()

        def peer(step):
            win = lax.rem(my_win + step // n_sta, n_win)
            sta = lax.rem(my_sta + lax.rem(step, n_sta), n_sta)
            return win, sta

        def greet(step, carry):
            pl.semaphore_signal(barrier, inc=1, device_id=peer(step), device_id_type=MESH_ID)
            return carry

        lax.fori_loop(1, n_all, greet, 0)

        def edge_copy(sig):
            return pltpu.make_async_remote_copy(
                src_ref=x_ref.at[sig, pl.ds(frame_count - halo_rows, halo_rows)],
                dst_ref=edge.at[sig],
                send_sem=edge_send.at[sig],
                recv_sem=edge_recv.at[sig],
                device_id=(my_win + 1, my_sta),
                device_id_type=MESH_ID,
            )

        def old_copy(sig):
            return pltpu.make_async_remote_copy(
                src_ref=spec.at[sig, pl.ds(fine_count * frame_rows, old_rows)],
                dst_ref=spec.at[sig, pl.ds(0, old_rows)],
                send_sem=old_send.at[sig],
                recv_sem=old_recv.at[sig],
                device_id=(my_win + 1, my_sta),
                device_id_type=MESH_ID,
            )

        def build_banded():
            taps = fine_ref[...].astype(jnp.float32)
            taps = jnp.concatenate([taps, taps], axis=1)
            place = lax.rem(lax.broadcasted_iota(jnp.int32, (2 * QUAD, frame_rows), 0), QUAD)
            for d in range(span):
                weights = jnp.zeros((2 * QUAD, frame_rows), jnp.float32)
                for gl in range(QUAD):
                    m = gl + fine_tap_count - 1 - d
                    if 0 <= m < fine_tap_count:
                        row = jnp.broadcast_to(taps[m : m + 1], weights.shape)
                        weights = jnp.where(place == gl, row, weights)
                table = table_ref[...].reshape(fine_len, 2 * QUAD, frame_rows)
                part = (table * weights[None]).reshape(fine_len * 2 * QUAD, frame_rows)
                banded[:, d * frame_rows : (d + 1) * frame_rows] = part.astype(jnp.bfloat16)

        def widen(sig):
            for k in range(cols):
                wide[k, pl.ds(halo_rows, frame_count)] = x_ref[
                    sig, :, pl.ds(k * 128, 128)
                ].astype(jnp.float32)

        def coarse_block(sig, i):
            pieces = []
            for k in range(cols):
                total = jnp.zeros((block, 128), jnp.float32)
                for m in range(tap_count):
                    row = coarse_ref[m : m + 1, k * 128 : (k + 1) * 128].astype(jnp.float32)
                    total = total + row * wide[k, pl.ds(i * block + halo_rows - m, block)]
                pieces.append(total.astype(jnp.bfloat16))
            windowed = jnp.concatenate(pieces, axis=1)
            result = jnp.dot(windowed, dft_ref[...], preferred_element_type=jnp.float32)
            result = result.astype(jnp.bfloat16)
            base = pl.multiple_of(old_rows + i * (block // fine_len) * frame_rows, frame_rows)
            for h in range(block // fine_len):
                for p in range(2):
                    spec[sig, pl.ds(base + (2 * h + p) * fine_len, fine_len)] = result[
                        h * fine_len : (h + 1) * fine_len, p * KEEP : (p + 1) * KEEP
                    ]

        def coarse(sig, first):
            widen(sig)

            def step(i, carry):
                coarse_block(sig, i)
                return carry

            lax.fori_loop(n_blocks // 2, n_blocks, step, 0)
            if first:
                pl.semaphore_wait(barrier, n_all - 1)

                @pl.when(my_win < n_win - 1)
                def _():
                    for s in range(sig_count):
                        edge_copy(s).start()

            @pl.when(my_win < n_win - 1)
            def _():
                old_copy(sig).start()

            lax.fori_loop(1, n_blocks // 2, step, 0)

            @pl.when(my_win > 0)
            def _():
                edge_copy(sig).wait_recv()
                for k in range(cols):
                    wide[k, pl.ds(0, halo_rows)] = edge[sig, :, pl.ds(k * 128, 128)].astype(
                        jnp.float32
                    )

            @pl.when(my_win == 0)
            def _():
                for k in range(cols):
                    wide[k, pl.ds(0, halo_rows)] = jnp.zeros((halo_rows, 128), jnp.float32)
                spec[sig, pl.ds(0, old_rows)] = jnp.zeros((old_rows, KEEP), jnp.bfloat16)

            coarse_block(sig, 0)

        lane = lax.broadcasted_iota(jnp.int32, (64, 128), 1)

        def fine(sig):
            @pl.when(my_win > 0)
            def _():
                old_copy(sig).wait_recv()

            for quad in range(n_quads):
                stage[quad] = jnp.dot(
                    banded[...],
                    spec[sig, pl.ds(quad * QUAD * frame_rows, span * frame_rows)],
                    preferred_element_type=jnp.float32,
                )

            def turn(i, carry):
                rows = pl.ds(pl.multiple_of(i * 64, 64), 64)
                a, b, c, d = [stage[quad, rows] for quad in range(4)]
                low = lane < 64
                a, c = (
                    jnp.where(low, a, pltpu.roll(c, 64, 1)),
                    jnp.where(low, pltpu.roll(a, 64, 1), c),
                )
                b, d = (
                    jnp.where(low, b, pltpu.roll(d, 64, 1)),
                    jnp.where(low, pltpu.roll(b, 64, 1), d),
                )
                even = lax.rem(lane, 64) < 32
                a, b = (
                    jnp.where(even, a, pltpu.roll(b, 32, 1)),
                    jnp.where(even, pltpu.roll(a, 96, 1), b),
                )
                c, d = (
                    jnp.where(even, c, pltpu.roll(d, 32, 1)),
                    jnp.where(even, pltpu.roll(c, 96, 1), d),
                )
                for win, value in enumerate((a, b, c, d)):
                    outbox[sig, pl.ds(win * n_sta + i * 8, 8)] = value.reshape(8, 8, 128).astype(jnp.bfloat16)
                return carry

            lax.fori_loop(0, fine_len // 8, turn, 0)

        def post(sig):
            mine = inbox.at[
                sig,
                my_sta // group,
                my_win,
                :,
                pl.ds(pl.multiple_of(lax.rem(my_sta, group) * 128, 128), 128),
            ]
            pltpu.make_async_copy(outbox.at[sig, my_win * n_sta + my_sta], mine, own_sem.at[sig]).start()

            def send(step, carry):
                win, sta = peer(step)
                pltpu.make_async_remote_copy(
                    src_ref=outbox.at[sig, win * n_sta + sta],
                    dst_ref=mine,
                    send_sem=send_sem.at[sig],
                    recv_sem=recv_sem.at[sig],
                    device_id=(win, sta),
                    device_id_type=MESH_ID,
                ).start()
                return carry

            lax.fori_loop(1, n_all, send, 0)

        def all_but_one(sig, sem):
            most = outbox.at[sig, pl.ds(0, n_all - 1)]
            pltpu.make_async_copy(most, most, sem).wait()

        def collect(sig):
            all_but_one(sig, recv_sem.at[sig])
            first = outbox.at[sig, 0]
            pltpu.make_async_copy(first, first, own_sem.at[sig]).wait()
            which = lax.rem(lax.broadcasted_iota(jnp.int32, (8 * n_win, group * 128), 1), 128) // 32

            def turn(i, carry):
                got = inbox[sig, i].astype(jnp.float32).reshape(n_win * 8, group * 128)
                spread = jnp.concatenate(
                    [
                        jnp.where(which == quad, got, 0.0).astype(jnp.bfloat16)
                        for quad in range(n_quads)
                    ],
                    axis=0,
                )
                value = lax.dot_general(
                    pick_ref[...], spread, NT_DIMS, preferred_element_type=jnp.float32
                )
                for c in range(band_local):
                    start = c * n_sta * sig_count + i * group * sig_count + sig
                    out_ref[pl.ds(start, group, stride=sig_count)] = value[
                        c * group : (c + 1) * group
                    ]
                return carry

            lax.fori_loop(0, n_groups, turn, 0)

        build_banded()
        coarse(0, True)
        for sig in range(sig_count):
            if sig + 1 < sig_count:
                coarse(sig + 1, False)
            fine(sig)
            post(sig)
        for sig in range(sig_count):
            collect(sig)
        for sig in range(sig_count):
            all_but_one(sig, send_sem.at[sig])

        @pl.when(my_win < n_win - 1)
        def _():
            for sig in range(sig_count):
                edge_copy(sig).wait_send()
                old_copy(sig).wait_send()

    dma = pltpu.SemaphoreType.DMA
    in_vmem = pl.BlockSpec(memory_space=pltpu.VMEM)
    bf16, f32 = jnp.bfloat16, jnp.float32
    return pl.pallas_call(
        kernel,
        out_shape=jax.ShapeDtypeStruct((band_local * n_sta * sig_count, 128), f32),
        in_specs=[in_vmem] * 6,
        out_specs=in_vmem,
        scratch_shapes=[
            pltpu.VMEM((cols, halo_rows + frame_count, 128), f32),
            pltpu.VMEM((sig_count, halo_rows, frame_len), bf16),
            pltpu.VMEM((sig_count, old_rows + fine_count * frame_rows, KEEP), bf16),
            pltpu.VMEM((fine_len * 2 * QUAD, span * frame_rows), bf16),
            pltpu.VMEM((n_quads, fine_len * 2 * QUAD, KEEP), f32),
            pltpu.VMEM((sig_count, n_all, 8, 128), bf16),
            pltpu.VMEM((sig_count, n_groups, n_win, 8, group * 128), bf16),
        ]
        + [dma((sig_count,))] * 7,
        compiler_params=pltpu.CompilerParams(
            collective_id=0, has_side_effects=True, vmem_limit_bytes=30 * 2**20
        ),
        name="channelise",
    )


def make_correlator(band_local, sig_all, scale):
    step = 4

    def kernel(x_ref, out_ref):
        part = lax.rem(lax.broadcasted_iota(jnp.int32, (sig_all, 128), 1), 8) < 4
        for c in range(step):
            x = x_ref[c]
            turned = jnp.where(part, pltpu.roll(x, 124, 1), -pltpu.roll(x, 4, 1))
            x = x.astype(jnp.bfloat16)
            turned = turned.astype(jnp.bfloat16)
            for index, left in enumerate((x, turned)):
                value = lax.dot_general(left, x, NT_DIMS, preferred_element_type=jnp.float32)
                out_ref[c, 0, index] = (value * scale).astype(jnp.bfloat16)

    return pl.pallas_call(
        kernel,
        grid=(band_local // step,),
        out_shape=jax.ShapeDtypeStruct((band_local, 1, 2, sig_all, sig_all), jnp.bfloat16),
        in_specs=[pl.BlockSpec((step, sig_all, 128), lambda i: (i, 0, 0))],
        out_specs=pl.BlockSpec((step, 1, 2, sig_all, sig_all), lambda i: (i, 0, 0, 0, 0)),
        compiler_params=pltpu.CompilerParams(vmem_limit_bytes=16 * 2**20),
        name="correlate",
    )


def per_device(samples, coarse_taps, fine_taps):
    n_win, n_sta = lax.axis_size("win"), lax.axis_size("sta")
    sig_local, samp_local = samples.shape
    tap_count, frame_len = coarse_taps.shape
    fine_tap_count, fine_len = fine_taps.shape
    frame_count = samp_local // frame_len
    band_local = KEEP // n_win
    frames = samples.reshape(sig_local, frame_count, frame_len)
    channelise = make_channeliser(
        n_win, n_sta, sig_local, frame_count, tap_count, frame_len, fine_tap_count, fine_len
    )
    fine = channelise(
        frames,
        coarse_taps,
        fine_taps,
        jnp.asarray(coarse_matrix(frame_len, KEEP)),
        jnp.asarray(fine_matrix(fine_len)),
        jnp.asarray(pick_matrix(band_local, 8, 128)),
    )
    frame_total = n_win * (frame_count // fine_len)
    correlate = make_correlator(band_local, n_sta * sig_local, 1.0 / frame_total)
    return correlate(fine.reshape(band_local, n_sta * sig_local, 128))


def solution(mesh):
    placed = (P("sta", "win"), P(), P())
    return jax.shard_map(
        per_device,
        mesh=mesh,
        in_specs=placed,
        out_specs=P("win", "sta", None, None, None),
        check_vma=False,
    )
```

```python
import math

import jax
import jax.numpy as jnp
import numpy as np
from jax import lax
from jax.experimental import pallas as pl
from jax.experimental.pallas import tpu as pltpu
from jax.sharding import PartitionSpec as P

KEEP = 128
QUAD = 4
MESH_ID = pl.DeviceIdType.MESH
NT_DIMS = (((1,), (1,)), ((), ()))


def coarse_matrix(frame_len, band_count):
    channels = frame_len // 8 + np.arange(band_count)
    angles = (np.arange(frame_len)[:, None] * channels[None, :]) % frame_len
    angles = angles.astype(np.float32) * np.float32(2.0 * math.pi / frame_len)
    return np.concatenate([np.cos(angles), -np.sin(angles)], axis=1).astype(jnp.bfloat16)


def fine_matrix(fine_len):
    angles = (np.arange(fine_len)[:, None] * np.arange(fine_len)[None, :]) % fine_len
    angles = angles.astype(np.float32) * np.float32(2.0 * math.pi / fine_len)
    cosines, sines = np.cos(angles), np.sin(angles)
    real_rows = np.concatenate([cosines, sines], axis=1)
    imag_rows = np.concatenate([-sines, cosines], axis=1)
    both = np.stack([real_rows, imag_rows], axis=1)
    return np.repeat(both.reshape(2 * fine_len, 2 * fine_len), QUAD, axis=0).astype(np.float32)


def pick_matrix(channels, senders, lanes):
    row = np.arange(channels * senders)
    col = np.arange(senders * lanes)
    same_sender = (row % senders)[:, None] == (col // lanes)[None, :]
    same_channel = (row // senders)[:, None] == (col % channels)[None, :]
    return (same_sender & same_channel).astype(jnp.bfloat16)


def make_channeliser(n_win, n_sta, sig_count, frame_count, tap_count, frame_len, fine_tap_count, fine_len):
    n_all = n_win * n_sta
    cols = frame_len // 128
    halo_rows = 16
    block = 128
    n_blocks = frame_count // block
    fine_count = frame_count // fine_len
    frame_rows = 2 * fine_len
    old_rows = (fine_tap_count - 1) * frame_rows
    span = fine_tap_count - 1 + QUAD
    n_quads = fine_count // QUAD
    band_local = KEEP // n_win
    group = 8
    n_groups = n_sta // group
    n_row = 16

    def kernel(
        x_ref, coarse_ref, fine_ref, dft_ref, table_ref, pick_ref, out_ref,
        wide, edge, spec, banded, stage, outbox, inbox,
        met, own_sem, edge_send, edge_recv, old_send, old_recv, send_sem, recv_sem,
    ):
        my_win = lax.axis_index("win")
        my_sta = lax.axis_index("sta")
        barrier = pltpu.get_barrier_semaphore()

        def peer(step):
            win = lax.rem(my_win + step // n_sta, n_win)
            sta = lax.rem(my_sta + lax.rem(step, n_sta), n_sta)
            return win, sta

        n_col = n_all // n_row
        sta_rows = n_sta // n_row
        my_col = my_win * sta_rows + my_sta // n_row
        my_row = lax.rem(my_sta, n_row)

        def along_row(step):
            return my_win, my_sta - my_row + lax.rem(my_row + step, n_row)

        def along_col(step):
            col = lax.rem(my_col + step, n_col)
            return col // sta_rows, lax.rem(col, sta_rows) * n_row + my_row

        def greet_row(step, carry):
            pl.semaphore_signal(barrier, inc=1, device_id=along_row(step), device_id_type=MESH_ID)
            return carry

        def greet_col(step, carry):
            pl.semaphore_signal(barrier, inc=1, device_id=along_col(step), device_id_type=MESH_ID)
            return carry

        def pass_on(step, carry):
            pl.semaphore_signal(met, inc=1, device_id=along_col(step), device_id_type=MESH_ID)
            return carry

        lax.fori_loop(1, n_row, greet_row, 0)
        lax.fori_loop(1, n_col, greet_col, 0)

        def edge_copy(sig):
            return pltpu.make_async_remote_copy(
                src_ref=x_ref.at[sig, pl.ds(frame_count - halo_rows, halo_rows)],
                dst_ref=edge.at[sig],
                send_sem=edge_send.at[sig],
                recv_sem=edge_recv.at[sig],
                device_id=(my_win + 1, my_sta),
                device_id_type=MESH_ID,
            )

        def old_copy(sig):
            return pltpu.make_async_remote_copy(
                src_ref=spec.at[sig, pl.ds(fine_count * frame_rows, old_rows)],
                dst_ref=spec.at[sig, pl.ds(0, old_rows)],
                send_sem=old_send.at[sig],
                recv_sem=old_recv.at[sig],
                device_id=(my_win + 1, my_sta),
                device_id_type=MESH_ID,
            )

        def build_banded():
            taps = fine_ref[...].astype(jnp.float32)
            taps = jnp.concatenate([taps, taps], axis=1)
            place = lax.rem(lax.broadcasted_iota(jnp.int32, (2 * QUAD, frame_rows), 0), QUAD)
            for d in range(span):
                weights = jnp.zeros((2 * QUAD, frame_rows), jnp.float32)
                for gl in range(QUAD):
                    m = gl + fine_tap_count - 1 - d
                    if 0 <= m < fine_tap_count:
                        row = jnp.broadcast_to(taps[m : m + 1], weights.shape)
                        weights = jnp.where(place == gl, row, weights)
                table = table_ref[...].reshape(fine_len, 2 * QUAD, frame_rows)
                part = (table * weights[None]).reshape(fine_len * 2 * QUAD, frame_rows)
                banded[:, d * frame_rows : (d + 1) * frame_rows] = part.astype(jnp.bfloat16)

        def widen(sig):
            for k in range(cols):
                wide[k, pl.ds(halo_rows, frame_count)] = x_ref[
                    sig, :, pl.ds(k * 128, 128)
                ].astype(jnp.float32)

        def coarse_block(sig, i):
            pieces = []
            for k in range(cols):
                total = jnp.zeros((block, 128), jnp.float32)
                for m in range(tap_count):
                    row = coarse_ref[m : m + 1, k * 128 : (k + 1) * 128].astype(jnp.float32)
                    total = total + row * wide[k, pl.ds(i * block + halo_rows - m, block)]
                pieces.append(total.astype(jnp.bfloat16))
            windowed = jnp.concatenate(pieces, axis=1)
            result = jnp.dot(windowed, dft_ref[...], preferred_element_type=jnp.float32)
            result = result.astype(jnp.bfloat16)
            base = pl.multiple_of(old_rows + i * (block // fine_len) * frame_rows, frame_rows)
            for h in range(block // fine_len):
                for p in range(2):
                    spec[sig, pl.ds(base + (2 * h + p) * fine_len, fine_len)] = result[
                        h * fine_len : (h + 1) * fine_len, p * KEEP : (p + 1) * KEEP
                    ]

        def coarse(sig, first):
            widen(sig)

            def step(i, carry):
                coarse_block(sig, i)
                return carry

            lax.fori_loop(n_blocks // 2, n_blocks, step, 0)
            if first:
                pl.semaphore_wait(met, n_col - 1)

                @pl.when(my_win < n_win - 1)
                def _():
                    for s in range(sig_count):
                        edge_copy(s).start()

            @pl.when(my_win < n_win - 1)
            def _():
                old_copy(sig).start()

            lax.fori_loop(1, n_blocks // 2, step, 0)

            @pl.when(my_win > 0)
            def _():
                edge_copy(sig).wait_recv()
                for k in range(cols):
                    wide[k, pl.ds(0, halo_rows)] = edge[sig, :, pl.ds(k * 128, 128)].astype(
                        jnp.float32
                    )

            @pl.when(my_win == 0)
            def _():
                for k in range(cols):
                    wide[k, pl.ds(0, halo_rows)] = jnp.zeros((halo_rows, 128), jnp.float32)
                spec[sig, pl.ds(0, old_rows)] = jnp.zeros((old_rows, KEEP), jnp.bfloat16)

            coarse_block(sig, 0)

        lane = lax.broadcasted_iota(jnp.int32, (64, 128), 1)

        def fine(sig):
            @pl.when(my_win > 0)
            def _():
                old_copy(sig).wait_recv()

            for quad in range(0, n_quads, 2):
                windows = [
                    spec[sig, pl.ds(q * QUAD * frame_rows, span * frame_rows)]
                    for q in (quad, quad + 1)
                ]
                result = jnp.dot(
                    banded[...],
                    jnp.concatenate(windows, axis=1),
                    preferred_element_type=jnp.float32,
                )
                stage[quad] = result[:, :KEEP]
                stage[quad + 1] = result[:, KEEP:]

            def turn(i, carry):
                rows = pl.ds(pl.multiple_of(i * 64, 64), 64)
                a, b, c, d = [stage[quad, rows] for quad in range(4)]
                low = lane < 64
                a, c = (
                    jnp.where(low, a, pltpu.roll(c, 64, 1)),
                    jnp.where(low, pltpu.roll(a, 64, 1), c),
                )
                b, d = (
                    jnp.where(low, b, pltpu.roll(d, 64, 1)),
                    jnp.where(low, pltpu.roll(b, 64, 1), d),
                )
                even = lax.rem(lane, 64) < 32
                a, b = (
                    jnp.where(even, a, pltpu.roll(b, 32, 1)),
                    jnp.where(even, pltpu.roll(a, 96, 1), b),
                )
                c, d = (
                    jnp.where(even, c, pltpu.roll(d, 32, 1)),
                    jnp.where(even, pltpu.roll(c, 96, 1), d),
                )
                for win, value in enumerate((a, b, c, d)):
                    outbox[sig, pl.ds(win * n_sta + i * 8, 8)] = value.reshape(8, 8, 128).astype(jnp.bfloat16)
                return carry

            lax.fori_loop(0, fine_len // 8, turn, 0)

        def post(sig):
            mine = inbox.at[
                sig,
                my_sta // group,
                my_win,
                :,
                pl.ds(pl.multiple_of(lax.rem(my_sta, group) * 128, 128), 128),
            ]
            pltpu.make_async_copy(outbox.at[sig, my_win * n_sta + my_sta], mine, own_sem.at[sig]).start()

            for turn in range(n_win):
                win = lax.rem(my_win + turn, n_win)
                first = 1 if turn == 0 else 0

                def send(step, carry, win=win):
                    sta = lax.rem(my_sta + step, n_sta)
                    pltpu.make_async_remote_copy(
                        src_ref=outbox.at[sig, win * n_sta + sta],
                        dst_ref=mine,
                        send_sem=send_sem.at[sig],
                        recv_sem=recv_sem.at[sig],
                        device_id=(win, sta),
                        device_id_type=MESH_ID,
                    ).start()
                    return carry

                lax.fori_loop(first, n_sta, send, 0, unroll=7 if first else 8)

        def all_but_one(sig, sem):
            most = outbox.at[sig, pl.ds(0, n_all - 1)]
            pltpu.make_async_copy(most, most, sem).wait()

        def collect(sig):
            all_but_one(sig, recv_sem.at[sig])
            first = outbox.at[sig, 0]
            pltpu.make_async_copy(first, first, own_sem.at[sig]).wait()
            which = lax.rem(lax.broadcasted_iota(jnp.int32, (8 * n_win, group * 128), 1), 128) // 32

            def turn(i, carry):
                spread = []
                for half in range(2):
                    got = inbox[sig, 2 * i + half].astype(jnp.float32)
                    got = got.reshape(n_win * 8, group * 128)
                    for quad in range(n_quads):
                        spread.append(jnp.where(which == quad, got, 0.0).astype(jnp.bfloat16))
                value = lax.dot_general(
                    pick_ref[...],
                    jnp.concatenate(spread, axis=0),
                    NT_DIMS,
                    preferred_element_type=jnp.float32,
                )
                for half in range(2):
                    for c in range(band_local):
                        start = c * n_sta * sig_count + (2 * i + half) * group * sig_count + sig
                        out_ref[pl.ds(start, group, stride=sig_count)] = value[
                            c * group : (c + 1) * group, half * 128 : (half + 1) * 128
                        ]
                return carry

            lax.fori_loop(0, n_groups // 2, turn, 0)

        build_banded()
        pl.semaphore_wait(barrier, n_row + n_col - 2)
        lax.fori_loop(1, n_col, pass_on, 0)
        coarse(0, True)
        fine(0)
        post(0)
        coarse(1, False)
        for sig in range(1, sig_count):
            if sig + 1 < sig_count:
                coarse(sig + 1, False)
            fine(sig)
            post(sig)
        for sig in range(sig_count):
            collect(sig)
        for sig in range(sig_count):
            all_but_one(sig, send_sem.at[sig])

        @pl.when(my_win < n_win - 1)
        def _():
            for sig in range(sig_count):
                edge_copy(sig).wait_send()
                old_copy(sig).wait_send()

    dma = pltpu.SemaphoreType.DMA
    in_vmem = pl.BlockSpec(memory_space=pltpu.VMEM)
    bf16, f32 = jnp.bfloat16, jnp.float32
    return pl.pallas_call(
        kernel,
        out_shape=jax.ShapeDtypeStruct((band_local * n_sta * sig_count, 128), f32),
        in_specs=[in_vmem] * 6,
        out_specs=in_vmem,
        scratch_shapes=[
            pltpu.VMEM((cols, halo_rows + frame_count, 128), f32),
            pltpu.VMEM((sig_count, halo_rows, frame_len), bf16),
            pltpu.VMEM((sig_count, old_rows + fine_count * frame_rows, KEEP), bf16),
            pltpu.VMEM((fine_len * 2 * QUAD, span * frame_rows), bf16),
            pltpu.VMEM((n_quads, fine_len * 2 * QUAD, KEEP), f32),
            pltpu.VMEM((sig_count, n_all, 8, 128), bf16),
            pltpu.VMEM((sig_count, n_groups, n_win, 8, group * 128), bf16),
        ]
        + [pltpu.SemaphoreType.REGULAR]
        + [dma((sig_count,))] * 7,
        compiler_params=pltpu.CompilerParams(
            collective_id=0, has_side_effects=True, vmem_limit_bytes=30 * 2**20
        ),
        name="channelise",
    )


def make_correlator(band_local, sig_all, scale):
    step = 4
    slots = 2
    n_steps = band_local // step

    def kernel(x_ref, out_ref, held, sems):
        part = lax.rem(lax.broadcasted_iota(jnp.int32, (sig_all, 128), 1), 8) < 4

        def put(i, slot):
            return pltpu.make_async_copy(
                held.at[slot], out_ref.at[pl.ds(i * step, step)], sems.at[slot]
            )

        def work(i, carry):
            slot = lax.rem(i, slots)

            @pl.when(i >= slots)
            def _():
                put(i - slots, slot).wait()

            for c in range(step):
                x = x_ref[i * step + c]
                turned = jnp.where(part, pltpu.roll(x, 124, 1), -pltpu.roll(x, 4, 1))
                x = x.astype(jnp.bfloat16)
                both = jnp.concatenate([x, turned.astype(jnp.bfloat16)], axis=0)
                value = lax.dot_general(both, x, NT_DIMS, preferred_element_type=jnp.float32)
                value = (value * scale).astype(jnp.bfloat16)
                held[slot, c, 0, 0] = value[:sig_all]
                held[slot, c, 0, 1] = value[sig_all:]
            put(i, slot).start()
            return carry

        lax.fori_loop(0, n_steps, work, 0)
        for i in range(n_steps - slots, n_steps):
            put(i, i % slots).wait()

    return pl.pallas_call(
        kernel,
        out_shape=jax.ShapeDtypeStruct((band_local, 1, 2, sig_all, sig_all), jnp.bfloat16),
        in_specs=[pl.BlockSpec(memory_space=pltpu.VMEM)],
        out_specs=pl.BlockSpec(memory_space=pl.ANY),
        scratch_shapes=[
            pltpu.VMEM((slots, step, 1, 2, sig_all, sig_all), jnp.bfloat16),
            pltpu.SemaphoreType.DMA((slots,)),
        ],
        compiler_params=pltpu.CompilerParams(vmem_limit_bytes=16 * 2**20),
        name="correlate",
    )


def per_device(samples, coarse_taps, fine_taps):
    n_win, n_sta = lax.axis_size("win"), lax.axis_size("sta")
    sig_local, samp_local = samples.shape
    tap_count, frame_len = coarse_taps.shape
    fine_tap_count, fine_len = fine_taps.shape
    frame_count = samp_local // frame_len
    band_local = KEEP // n_win
    frames = samples.reshape(sig_local, frame_count, frame_len)
    channelise = make_channeliser(
        n_win, n_sta, sig_local, frame_count, tap_count, frame_len, fine_tap_count, fine_len
    )
    fine = channelise(
        frames,
        coarse_taps,
        fine_taps,
        jnp.asarray(coarse_matrix(frame_len, KEEP)),
        jnp.asarray(fine_matrix(fine_len)),
        jnp.asarray(pick_matrix(band_local, 8, 128)),
    )
    frame_total = n_win * (frame_count // fine_len)
    correlate = make_correlator(band_local, n_sta * sig_local, 1.0 / frame_total)
    return correlate(fine.reshape(band_local, n_sta * sig_local, 128))


def solution(mesh):
    placed = (P("sta", "win"), P(), P())
    return jax.shard_map(
        per_device,
        mesh=mesh,
        in_specs=placed,
        out_specs=P("win", "sta", None, None, None),
        check_vma=False,
    )
```

```python
import math

import jax
import jax.numpy as jnp
import numpy as np
from jax import lax
from jax.experimental import pallas as pl
from jax.experimental.pallas import tpu as pltpu
from jax.sharding import PartitionSpec as P

KEEP = 128
QUAD = 4
MESH_ID = pl.DeviceIdType.MESH
NT_DIMS = (((1,), (1,)), ((), ()))


def coarse_matrix(frame_len, band_count):
    channels = frame_len // 8 + np.arange(band_count)
    angles = (np.arange(frame_len)[:, None] * channels[None, :]) % frame_len
    angles = angles.astype(np.float32) * np.float32(2.0 * math.pi / frame_len)
    return np.concatenate([np.cos(angles), -np.sin(angles)], axis=1).astype(jnp.bfloat16)


def fine_matrix(fine_len):
    angles = (np.arange(fine_len)[:, None] * np.arange(fine_len)[None, :]) % fine_len
    angles = angles.astype(np.float32) * np.float32(2.0 * math.pi / fine_len)
    cosines, sines = np.cos(angles), np.sin(angles)
    real_rows = np.concatenate([cosines, sines], axis=1)
    imag_rows = np.concatenate([-sines, cosines], axis=1)
    both = np.stack([real_rows, imag_rows], axis=1)
    return np.repeat(both.reshape(2 * fine_len, 2 * fine_len), QUAD, axis=0).astype(np.float32)


def pick_matrix(channels, senders, lanes):
    row = np.arange(channels * senders)
    col = np.arange(senders * lanes)
    same_sender = (row % senders)[:, None] == (col // lanes)[None, :]
    same_channel = (row // senders)[:, None] == (col % channels)[None, :]
    return (same_sender & same_channel).astype(jnp.bfloat16)


def make_channeliser(n_win, n_sta, sig_count, frame_count, tap_count, frame_len, fine_tap_count, fine_len):
    n_all = n_win * n_sta
    cols = frame_len // 128
    halo_rows = 16
    block = 128
    n_blocks = frame_count // block
    fine_count = frame_count // fine_len
    frame_rows = 2 * fine_len
    old_rows = (fine_tap_count - 1) * frame_rows
    span = fine_tap_count - 1 + QUAD
    n_quads = fine_count // QUAD
    band_local = KEEP // n_win
    group = 8
    n_groups = n_sta // group
    n_row = 16

    def kernel(
        x_ref, coarse_ref, fine_ref, dft_ref, table_ref, pick_ref, out_ref,
        wide, edge, spec, banded, stage, outbox, inbox,
        met, own_sem, edge_send, edge_recv, old_send, old_recv, send_sem, recv_sem,
    ):
        my_win = lax.axis_index("win")
        my_sta = lax.axis_index("sta")
        barrier = pltpu.get_barrier_semaphore()

        def peer(step):
            win = lax.rem(my_win + step // n_sta, n_win)
            sta = lax.rem(my_sta + lax.rem(step, n_sta), n_sta)
            return win, sta

        n_col = n_all // n_row
        sta_rows = n_sta // n_row
        my_col = my_win * sta_rows + my_sta // n_row
        my_row = lax.rem(my_sta, n_row)

        def along_row(step):
            return my_win, my_sta - my_row + lax.rem(my_row + step, n_row)

        def along_col(step):
            col = lax.rem(my_col + step, n_col)
            return col // sta_rows, lax.rem(col, sta_rows) * n_row + my_row

        def greet_row(step, carry):
            pl.semaphore_signal(barrier, inc=1, device_id=along_row(step), device_id_type=MESH_ID)
            return carry

        def greet_col(step, carry):
            pl.semaphore_signal(barrier, inc=1, device_id=along_col(step), device_id_type=MESH_ID)
            return carry

        def pass_on(step, carry):
            pl.semaphore_signal(met, inc=1, device_id=along_col(step), device_id_type=MESH_ID)
            return carry

        lax.fori_loop(1, n_row, greet_row, 0)
        lax.fori_loop(1, n_col, greet_col, 0)

        def edge_copy(sig):
            return pltpu.make_async_remote_copy(
                src_ref=x_ref.at[sig, pl.ds(frame_count - halo_rows, halo_rows)],
                dst_ref=edge.at[sig],
                send_sem=edge_send.at[sig],
                recv_sem=edge_recv.at[sig],
                device_id=(my_win + 1, my_sta),
                device_id_type=MESH_ID,
            )

        def old_copy(sig):
            return pltpu.make_async_remote_copy(
                src_ref=spec.at[sig, pl.ds(fine_count * frame_rows, old_rows)],
                dst_ref=spec.at[sig, pl.ds(0, old_rows)],
                send_sem=old_send.at[sig],
                recv_sem=old_recv.at[sig],
                device_id=(my_win + 1, my_sta),
                device_id_type=MESH_ID,
            )

        def build_banded():
            taps = fine_ref[...].astype(jnp.float32)
            taps = jnp.concatenate([taps, taps], axis=1)
            place = lax.rem(lax.broadcasted_iota(jnp.int32, (2 * QUAD, frame_rows), 0), QUAD)
            for d in range(span):
                weights = jnp.zeros((2 * QUAD, frame_rows), jnp.float32)
                for gl in range(QUAD):
                    m = gl + fine_tap_count - 1 - d
                    if 0 <= m < fine_tap_count:
                        row = jnp.broadcast_to(taps[m : m + 1], weights.shape)
                        weights = jnp.where(place == gl, row, weights)
                table = table_ref[...].reshape(fine_len, 2 * QUAD, frame_rows)
                part = (table * weights[None]).reshape(fine_len * 2 * QUAD, frame_rows)
                banded[:, d * frame_rows : (d + 1) * frame_rows] = part.astype(jnp.bfloat16)

        def widen(sig):
            for k in range(cols):
                wide[k, pl.ds(halo_rows, frame_count)] = x_ref[
                    sig, :, pl.ds(k * 128, 128)
                ].astype(jnp.float32)

        def coarse_block(sig, i):
            pieces = []
            for k in range(cols):
                total = jnp.zeros((block, 128), jnp.float32)
                for m in range(tap_count):
                    row = coarse_ref[m : m + 1, k * 128 : (k + 1) * 128].astype(jnp.float32)
                    total = total + row * wide[k, pl.ds(i * block + halo_rows - m, block)]
                pieces.append(total.astype(jnp.bfloat16))
            windowed = jnp.concatenate(pieces, axis=1)
            result = jnp.dot(windowed, dft_ref[...], preferred_element_type=jnp.float32)
            result = result.astype(jnp.bfloat16)
            base = pl.multiple_of(old_rows + i * (block // fine_len) * frame_rows, frame_rows)
            for h in range(block // fine_len):
                for p in range(2):
                    spec[sig, pl.ds(base + (2 * h + p) * fine_len, fine_len)] = result[
                        h * fine_len : (h + 1) * fine_len, p * KEEP : (p + 1) * KEEP
                    ]

        def coarse(sig, first):
            widen(sig)

            def step(i, carry):
                coarse_block(sig, i)
                return carry

            lax.fori_loop(n_blocks // 2, n_blocks, step, 0)
            if first:
                pl.semaphore_wait(barrier, n_row + n_col - 2)
                lax.fori_loop(1, n_col, pass_on, 0)

            @pl.when(my_win < n_win - 1)
            def _():
                if first:
                    edge_copy(0).start()
                old_copy(sig).start()
                if first:
                    for s in range(1, sig_count):
                        edge_copy(s).start()

            lax.fori_loop(1, n_blocks // 2, step, 0)

            @pl.when(my_win > 0)
            def _():
                edge_copy(sig).wait_recv()
                for k in range(cols):
                    wide[k, pl.ds(0, halo_rows)] = edge[sig, :, pl.ds(k * 128, 128)].astype(
                        jnp.float32
                    )

            @pl.when(my_win == 0)
            def _():
                for k in range(cols):
                    wide[k, pl.ds(0, halo_rows)] = jnp.zeros((halo_rows, 128), jnp.float32)
                spec[sig, pl.ds(0, old_rows)] = jnp.zeros((old_rows, KEEP), jnp.bfloat16)

            coarse_block(sig, 0)

        lane = lax.broadcasted_iota(jnp.int32, (64, 128), 1)

        def fine(sig):
            @pl.when(my_win > 0)
            def _():
                old_copy(sig).wait_recv()

            for quad in range(0, n_quads, 2):
                windows = [
                    spec[sig, pl.ds(q * QUAD * frame_rows, span * frame_rows)]
                    for q in (quad, quad + 1)
                ]
                result = jnp.dot(
                    banded[...],
                    jnp.concatenate(windows, axis=1),
                    preferred_element_type=jnp.float32,
                )
                stage[quad] = result[:, :KEEP]
                stage[quad + 1] = result[:, KEEP:]

            def turn(i, carry):
                rows = pl.ds(pl.multiple_of(i * 64, 64), 64)
                a, b, c, d = [stage[quad, rows] for quad in range(4)]
                low = lane < 64
                a, c = (
                    jnp.where(low, a, pltpu.roll(c, 64, 1)),
                    jnp.where(low, pltpu.roll(a, 64, 1), c),
                )
                b, d = (
                    jnp.where(low, b, pltpu.roll(d, 64, 1)),
                    jnp.where(low, pltpu.roll(b, 64, 1), d),
                )
                even = lax.rem(lane, 64) < 32
                a, b = (
                    jnp.where(even, a, pltpu.roll(b, 32, 1)),
                    jnp.where(even, pltpu.roll(a, 96, 1), b),
                )
                c, d = (
                    jnp.where(even, c, pltpu.roll(d, 32, 1)),
                    jnp.where(even, pltpu.roll(c, 96, 1), d),
                )
                for win, value in enumerate((a, b, c, d)):
                    outbox[sig, pl.ds(win * n_sta + i * 8, 8)] = value.reshape(8, 8, 128).astype(jnp.bfloat16)
                return carry

            lax.fori_loop(0, fine_len // 8, turn, 0)

        def post(sig):
            mine = inbox.at[
                sig,
                my_sta // group,
                my_win,
                :,
                pl.ds(pl.multiple_of(lax.rem(my_sta, group) * 128, 128), 128),
            ]
            pltpu.make_async_copy(outbox.at[sig, my_win * n_sta + my_sta], mine, own_sem.at[sig]).start()

            for turn in range(n_win):
                win = lax.rem(my_win + turn, n_win)
                first = 1 if turn == 0 else 0

                def send(step, carry, win=win):
                    sta = lax.rem(my_sta + step, n_sta)
                    pltpu.make_async_remote_copy(
                        src_ref=outbox.at[sig, win * n_sta + sta],
                        dst_ref=mine,
                        send_sem=send_sem.at[sig],
                        recv_sem=recv_sem.at[sig],
                        device_id=(win, sta),
                        device_id_type=MESH_ID,
                    ).start()
                    return carry

                lax.fori_loop(first, n_sta, send, 0, unroll=7 if first else 8)

        def all_but_one(sig, sem):
            most = outbox.at[sig, pl.ds(0, n_all - 1)]
            pltpu.make_async_copy(most, most, sem).wait()

        def collect(sig):
            all_but_one(sig, recv_sem.at[sig])
            first = outbox.at[sig, 0]
            pltpu.make_async_copy(first, first, own_sem.at[sig]).wait()
            which = lax.rem(lax.broadcasted_iota(jnp.int32, (8 * n_win, group * 128), 1), 128) // 32

            def turn(i, carry):
                spread = []
                for half in range(2):
                    got = inbox[sig, 2 * i + half].astype(jnp.float32)
                    got = got.reshape(n_win * 8, group * 128)
                    for quad in range(n_quads):
                        spread.append(jnp.where(which == quad, got, 0.0).astype(jnp.bfloat16))
                value = lax.dot_general(
                    pick_ref[...],
                    jnp.concatenate(spread, axis=0),
                    NT_DIMS,
                    preferred_element_type=jnp.float32,
                )
                for half in range(2):
                    for c in range(band_local):
                        start = c * n_sta * sig_count + (2 * i + half) * group * sig_count + sig
                        out_ref[pl.ds(start, group, stride=sig_count)] = value[
                            c * group : (c + 1) * group, half * 128 : (half + 1) * 128
                        ]
                return carry

            lax.fori_loop(0, n_groups // 2, turn, 0)

        build_banded()
        coarse(0, True)
        fine(0)
        pl.semaphore_wait(met, n_col - 1)
        post(0)
        coarse(1, False)
        for sig in range(1, sig_count):
            if sig + 1 < sig_count:
                coarse(sig + 1, False)
            fine(sig)
            post(sig)
        for sig in range(sig_count):
            collect(sig)
        for sig in range(sig_count):
            all_but_one(sig, send_sem.at[sig])

        @pl.when(my_win < n_win - 1)
        def _():
            for sig in range(sig_count):
                edge_copy(sig).wait_send()
                old_copy(sig).wait_send()

    dma = pltpu.SemaphoreType.DMA
    in_vmem = pl.BlockSpec(memory_space=pltpu.VMEM)
    bf16, f32 = jnp.bfloat16, jnp.float32
    return pl.pallas_call(
        kernel,
        out_shape=jax.ShapeDtypeStruct((band_local * n_sta * sig_count, 128), f32),
        in_specs=[in_vmem] * 6,
        out_specs=in_vmem,
        scratch_shapes=[
            pltpu.VMEM((cols, halo_rows + frame_count, 128), f32),
            pltpu.VMEM((sig_count, halo_rows, frame_len), bf16),
            pltpu.VMEM((sig_count, old_rows + fine_count * frame_rows, KEEP), bf16),
            pltpu.VMEM((fine_len * 2 * QUAD, span * frame_rows), bf16),
            pltpu.VMEM((n_quads, fine_len * 2 * QUAD, KEEP), f32),
            pltpu.VMEM((sig_count, n_all, 8, 128), bf16),
            pltpu.VMEM((sig_count, n_groups, n_win, 8, group * 128), bf16),
        ]
        + [pltpu.SemaphoreType.REGULAR]
        + [dma((sig_count,))] * 7,
        compiler_params=pltpu.CompilerParams(
            collective_id=0, has_side_effects=True, vmem_limit_bytes=30 * 2**20
        ),
        name="channelise",
    )


def make_correlator(band_local, sig_all, scale):
    step = 4
    slots = 4
    n_steps = band_local // step

    def kernel(x_ref, out_ref, held, sems):
        part = lax.rem(lax.broadcasted_iota(jnp.int32, (sig_all, 128), 1), 8) < 4

        def put(i, slot):
            return pltpu.make_async_copy(
                held.at[slot], out_ref.at[pl.ds(i * step, step)], sems.at[slot]
            )

        def work(i, carry):
            slot = lax.rem(i, slots)

            @pl.when(i >= slots)
            def _():
                put(i - slots, slot).wait()

            for c in range(step):
                x = x_ref[i * step + c]
                turned = jnp.where(part, pltpu.roll(x, 124, 1), -pltpu.roll(x, 4, 1))
                x = x.astype(jnp.bfloat16)
                both = jnp.concatenate([x, turned.astype(jnp.bfloat16)], axis=0)
                value = lax.dot_general(both, x, NT_DIMS, preferred_element_type=jnp.float32)
                value = (value * scale).astype(jnp.bfloat16)
                held[slot, c, 0, 0] = value[:sig_all]
                held[slot, c, 0, 1] = value[sig_all:]
            put(i, slot).start()
            return carry

        lax.fori_loop(0, n_steps, work, 0)
        for i in range(n_steps - slots, n_steps):
            put(i, i % slots).wait()

    return pl.pallas_call(
        kernel,
        out_shape=jax.ShapeDtypeStruct((band_local, 1, 2, sig_all, sig_all), jnp.bfloat16),
        in_specs=[pl.BlockSpec(memory_space=pltpu.VMEM)],
        out_specs=pl.BlockSpec(memory_space=pl.ANY),
        scratch_shapes=[
            pltpu.VMEM((slots, step, 1, 2, sig_all, sig_all), jnp.bfloat16),
            pltpu.SemaphoreType.DMA((slots,)),
        ],
        compiler_params=pltpu.CompilerParams(vmem_limit_bytes=16 * 2**20),
        name="correlate",
    )


def per_device(samples, coarse_taps, fine_taps):
    n_win, n_sta = lax.axis_size("win"), lax.axis_size("sta")
    sig_local, samp_local = samples.shape
    tap_count, frame_len = coarse_taps.shape
    fine_tap_count, fine_len = fine_taps.shape
    frame_count = samp_local // frame_len
    band_local = KEEP // n_win
    frames = samples.reshape(sig_local, frame_count, frame_len)
    channelise = make_channeliser(
        n_win, n_sta, sig_local, frame_count, tap_count, frame_len, fine_tap_count, fine_len
    )
    fine = channelise(
        frames,
        coarse_taps,
        fine_taps,
        jnp.asarray(coarse_matrix(frame_len, KEEP)),
        jnp.asarray(fine_matrix(fine_len)),
        jnp.asarray(pick_matrix(band_local, 8, 128)),
    )
    frame_total = n_win * (frame_count // fine_len)
    correlate = make_correlator(band_local, n_sta * sig_local, 1.0 / frame_total)
    return correlate(fine.reshape(band_local, n_sta * sig_local, 128))


def solution(mesh):
    placed = (P("sta", "win"), P(), P())
    return jax.shard_map(
        per_device,
        mesh=mesh,
        in_specs=placed,
        out_specs=P("win", "sta", None, None, None),
        check_vma=False,
    )
```

```python
import math

import jax
import jax.numpy as jnp
import numpy as np
from jax import lax
from jax.experimental import pallas as pl
from jax.experimental.pallas import tpu as pltpu
from jax.sharding import PartitionSpec as P

KEEP = 128
QUAD = 4
MESH_ID = pl.DeviceIdType.MESH
NT_DIMS = (((1,), (1,)), ((), ()))


def coarse_matrix(frame_len, band_count):
    channels = frame_len // 8 + np.arange(band_count)
    angles = (np.arange(frame_len)[:, None] * channels[None, :]) % frame_len
    angles = angles.astype(np.float32) * np.float32(2.0 * math.pi / frame_len)
    return np.concatenate([np.cos(angles), -np.sin(angles)], axis=1).astype(jnp.bfloat16)


def fine_matrix(fine_len):
    angles = (np.arange(fine_len)[:, None] * np.arange(fine_len)[None, :]) % fine_len
    angles = angles.astype(np.float32) * np.float32(2.0 * math.pi / fine_len)
    cosines, sines = np.cos(angles), np.sin(angles)
    real_rows = np.concatenate([cosines, sines], axis=1)
    imag_rows = np.concatenate([-sines, cosines], axis=1)
    both = np.stack([real_rows, imag_rows], axis=1)
    return np.repeat(both.reshape(2 * fine_len, 2 * fine_len), QUAD, axis=0).astype(np.float32)


def pick_matrix(channels, senders, lanes):
    row = np.arange(channels * senders)
    col = np.arange(senders * lanes)
    same_sender = (row % senders)[:, None] == (col // lanes)[None, :]
    same_channel = (row // senders)[:, None] == (col % channels)[None, :]
    return (same_sender & same_channel).astype(jnp.bfloat16)


def make_channeliser(n_win, n_sta, sig_count, frame_count, tap_count, frame_len, fine_tap_count, fine_len):
    n_all = n_win * n_sta
    cols = frame_len // 128
    halo_rows = 16
    block = 128
    n_blocks = frame_count // block
    fine_count = frame_count // fine_len
    frame_rows = 2 * fine_len
    old_rows = (fine_tap_count - 1) * frame_rows
    span = fine_tap_count - 1 + QUAD
    n_quads = fine_count // QUAD
    band_local = KEEP // n_win
    group = 8
    n_groups = n_sta // group
    n_row = 16

    def kernel(
        x_ref, coarse_ref, fine_ref, dft_ref, table_ref, pick_ref, out_ref,
        wide, edge, spec, banded, stage, outbox, inbox,
        met, own_sem, edge_send, edge_recv, old_send, old_recv, send_sem, recv_sem,
    ):
        my_win = lax.axis_index("win")
        my_sta = lax.axis_index("sta")
        barrier = pltpu.get_barrier_semaphore()

        def peer(step):
            win = lax.rem(my_win + step // n_sta, n_win)
            sta = lax.rem(my_sta + lax.rem(step, n_sta), n_sta)
            return win, sta

        n_col = n_all // n_row
        sta_rows = n_sta // n_row
        my_col = my_win * sta_rows + my_sta // n_row
        my_row = lax.rem(my_sta, n_row)

        def along_row(step):
            return my_win, my_sta - my_row + lax.rem(my_row + step, n_row)

        def along_col(step):
            col = lax.rem(my_col + step, n_col)
            return col // sta_rows, lax.rem(col, sta_rows) * n_row + my_row

        def greet_row(step, carry):
            pl.semaphore_signal(barrier, inc=1, device_id=along_row(step), device_id_type=MESH_ID)
            return carry

        def greet_col(step, carry):
            pl.semaphore_signal(barrier, inc=1, device_id=along_col(step), device_id_type=MESH_ID)
            return carry

        def pass_on(step, carry):
            pl.semaphore_signal(met, inc=1, device_id=along_col(step), device_id_type=MESH_ID)
            return carry

        lax.fori_loop(1, n_row, greet_row, 0)
        lax.fori_loop(1, n_col, greet_col, 0)

        def edge_copy(sig):
            return pltpu.make_async_remote_copy(
                src_ref=x_ref.at[sig, pl.ds(frame_count - halo_rows, halo_rows)],
                dst_ref=edge.at[sig],
                send_sem=edge_send.at[sig],
                recv_sem=edge_recv.at[sig],
                device_id=(my_win + 1, my_sta),
                device_id_type=MESH_ID,
            )

        def old_copy(sig):
            return pltpu.make_async_remote_copy(
                src_ref=spec.at[sig, pl.ds(fine_count * frame_rows, old_rows)],
                dst_ref=spec.at[sig, pl.ds(0, old_rows)],
                send_sem=old_send.at[sig],
                recv_sem=old_recv.at[sig],
                device_id=(my_win + 1, my_sta),
                device_id_type=MESH_ID,
            )

        def build_banded():
            taps = fine_ref[...].astype(jnp.float32)
            taps = jnp.concatenate([taps, taps], axis=1)
            place = lax.rem(lax.broadcasted_iota(jnp.int32, (2 * QUAD, frame_rows), 0), QUAD)
            for d in range(span):
                weights = jnp.zeros((2 * QUAD, frame_rows), jnp.float32)
                for gl in range(QUAD):
                    m = gl + fine_tap_count - 1 - d
                    if 0 <= m < fine_tap_count:
                        row = jnp.broadcast_to(taps[m : m + 1], weights.shape)
                        weights = jnp.where(place == gl, row, weights)
                table = table_ref[...].reshape(fine_len, 2 * QUAD, frame_rows)
                part = (table * weights[None]).reshape(fine_len * 2 * QUAD, frame_rows)
                banded[:, d * frame_rows : (d + 1) * frame_rows] = part.astype(jnp.bfloat16)

        def widen(sig):
            for k in range(cols):
                wide[k, pl.ds(halo_rows, frame_count)] = x_ref[
                    sig, :, pl.ds(k * 128, 128)
                ].astype(jnp.float32)

        def coarse_block(sig, i):
            pieces = []
            for k in range(cols):
                total = jnp.zeros((block, 128), jnp.float32)
                for m in range(tap_count):
                    row = coarse_ref[m : m + 1, k * 128 : (k + 1) * 128].astype(jnp.float32)
                    total = total + row * wide[k, pl.ds(i * block + halo_rows - m, block)]
                pieces.append(total.astype(jnp.bfloat16))
            windowed = jnp.concatenate(pieces, axis=1)
            result = jnp.dot(windowed, dft_ref[...], preferred_element_type=jnp.float32)
            result = result.astype(jnp.bfloat16)
            base = pl.multiple_of(old_rows + i * (block // fine_len) * frame_rows, frame_rows)
            for h in range(block // fine_len):
                for p in range(2):
                    spec[sig, pl.ds(base + (2 * h + p) * fine_len, fine_len)] = result[
                        h * fine_len : (h + 1) * fine_len, p * KEEP : (p + 1) * KEEP
                    ]

        def coarse(sig, first):
            widen(sig)

            def step(i, carry):
                coarse_block(sig, i)
                return carry

            lax.fori_loop(n_blocks // 2, n_blocks, step, 0)
            if first:
                pl.semaphore_wait(barrier, n_row + n_col - 2)
                lax.fori_loop(1, n_col, pass_on, 0)

            @pl.when(my_win < n_win - 1)
            def _():
                if first:
                    edge_copy(0).start()
                old_copy(sig).start()
                if first:
                    for s in range(1, sig_count):
                        edge_copy(s).start()

            lax.fori_loop(1, n_blocks // 2, step, 0)

            @pl.when(my_win > 0)
            def _():
                edge_copy(sig).wait_recv()
                for k in range(cols):
                    wide[k, pl.ds(0, halo_rows)] = edge[sig, :, pl.ds(k * 128, 128)].astype(
                        jnp.float32
                    )

            @pl.when(my_win == 0)
            def _():
                for k in range(cols):
                    wide[k, pl.ds(0, halo_rows)] = jnp.zeros((halo_rows, 128), jnp.float32)
                spec[sig, pl.ds(0, old_rows)] = jnp.zeros((old_rows, KEEP), jnp.bfloat16)

            coarse_block(sig, 0)

        lane = lax.broadcasted_iota(jnp.int32, (64, 128), 1)

        def fine(sig):
            @pl.when(my_win > 0)
            def _():
                old_copy(sig).wait_recv()

            for quad in range(0, n_quads, 2):
                windows = [
                    spec[sig, pl.ds(q * QUAD * frame_rows, span * frame_rows)]
                    for q in (quad, quad + 1)
                ]
                result = jnp.dot(
                    banded[...],
                    jnp.concatenate(windows, axis=1),
                    preferred_element_type=jnp.float32,
                )
                stage[quad] = result[:, :KEEP]
                stage[quad + 1] = result[:, KEEP:]

            def turn(i, carry):
                rows = pl.ds(pl.multiple_of(i * 64, 64), 64)
                a, b, c, d = [stage[quad, rows] for quad in range(4)]
                low = lane < 64
                a, c = (
                    jnp.where(low, a, pltpu.roll(c, 64, 1)),
                    jnp.where(low, pltpu.roll(a, 64, 1), c),
                )
                b, d = (
                    jnp.where(low, b, pltpu.roll(d, 64, 1)),
                    jnp.where(low, pltpu.roll(b, 64, 1), d),
                )
                even = lax.rem(lane, 64) < 32
                a, b = (
                    jnp.where(even, a, pltpu.roll(b, 32, 1)),
                    jnp.where(even, pltpu.roll(a, 96, 1), b),
                )
                c, d = (
                    jnp.where(even, c, pltpu.roll(d, 32, 1)),
                    jnp.where(even, pltpu.roll(c, 96, 1), d),
                )
                for win, value in enumerate((a, b, c, d)):
                    outbox[sig, pl.ds(win * n_sta + i * 8, 8)] = value.reshape(8, 8, 128).astype(jnp.bfloat16)
                return carry

            lax.fori_loop(0, fine_len // 8, turn, 0)

        def post(sig):
            mine = inbox.at[
                sig,
                my_sta // group,
                my_win,
                :,
                pl.ds(pl.multiple_of(lax.rem(my_sta, group) * 128, 128), 128),
            ]
            pltpu.make_async_copy(outbox.at[sig, my_win * n_sta + my_sta], mine, own_sem.at[sig]).start()

            for turn in range(n_win):
                win = lax.rem(my_win + turn, n_win)
                first = 1 if turn == 0 else 0

                def send(step, carry, win=win):
                    sta = lax.rem(my_sta + step, n_sta)
                    pltpu.make_async_remote_copy(
                        src_ref=outbox.at[sig, win * n_sta + sta],
                        dst_ref=mine,
                        send_sem=send_sem.at[sig],
                        recv_sem=recv_sem.at[sig],
                        device_id=(win, sta),
                        device_id_type=MESH_ID,
                    ).start()
                    return carry

                lax.fori_loop(first, n_sta, send, 0, unroll=7 if first else 8)

        def all_but_one(sig, sem):
            most = outbox.at[sig, pl.ds(0, n_all - 1)]
            pltpu.make_async_copy(most, most, sem).wait()

        def collect(sig):
            all_but_one(sig, recv_sem.at[sig])
            first = outbox.at[sig, 0]
            pltpu.make_async_copy(first, first, own_sem.at[sig]).wait()
            which = lax.rem(lax.broadcasted_iota(jnp.int32, (8 * n_win, group * 128), 1), 128) // 32

            def turn(i, carry):
                spread = []
                for half in range(2):
                    got = inbox[sig, 2 * i + half].astype(jnp.float32)
                    got = got.reshape(n_win * 8, group * 128)
                    for quad in range(n_quads):
                        spread.append(jnp.where(which == quad, got, 0.0).astype(jnp.bfloat16))
                value = lax.dot_general(
                    pick_ref[...],
                    jnp.concatenate(spread, axis=0),
                    NT_DIMS,
                    preferred_element_type=jnp.float32,
                )
                for half in range(2):
                    for c in range(band_local):
                        start = c * n_sta * sig_count + (2 * i + half) * group * sig_count + sig
                        out_ref[pl.ds(start, group, stride=sig_count)] = value[
                            c * group : (c + 1) * group, half * 128 : (half + 1) * 128
                        ]
                return carry

            lax.fori_loop(0, n_groups // 2, turn, 0)

        coarse(0, True)
        build_banded()
        fine(0)
        pl.semaphore_wait(met, n_col - 1)
        post(0)
        coarse(1, False)
        for sig in range(1, sig_count):
            if sig + 1 < sig_count:
                coarse(sig + 1, False)
            fine(sig)
            post(sig)
        for sig in range(sig_count):
            collect(sig)
        for sig in range(sig_count):
            all_but_one(sig, send_sem.at[sig])

        @pl.when(my_win < n_win - 1)
        def _():
            for sig in range(sig_count):
                edge_copy(sig).wait_send()
                old_copy(sig).wait_send()

    dma = pltpu.SemaphoreType.DMA
    in_vmem = pl.BlockSpec(memory_space=pltpu.VMEM)
    bf16, f32 = jnp.bfloat16, jnp.float32
    return pl.pallas_call(
        kernel,
        out_shape=jax.ShapeDtypeStruct((band_local * n_sta * sig_count, 128), f32),
        in_specs=[in_vmem] * 6,
        out_specs=in_vmem,
        scratch_shapes=[
            pltpu.VMEM((cols, halo_rows + frame_count, 128), f32),
            pltpu.VMEM((sig_count, halo_rows, frame_len), bf16),
            pltpu.VMEM((sig_count, old_rows + fine_count * frame_rows, KEEP), bf16),
            pltpu.VMEM((fine_len * 2 * QUAD, span * frame_rows), bf16),
            pltpu.VMEM((n_quads, fine_len * 2 * QUAD, KEEP), f32),
            pltpu.VMEM((sig_count, n_all, 8, 128), bf16),
            pltpu.VMEM((sig_count, n_groups, n_win, 8, group * 128), bf16),
        ]
        + [pltpu.SemaphoreType.REGULAR]
        + [dma((sig_count,))] * 7,
        compiler_params=pltpu.CompilerParams(
            collective_id=0, has_side_effects=True, vmem_limit_bytes=30 * 2**20
        ),
        name="channelise",
    )


def make_correlator(band_local, sig_all, scale):
    step = 4
    slots = 4
    n_steps = band_local // step

    def kernel(x_ref, out_ref, held, sems):
        part = lax.rem(lax.broadcasted_iota(jnp.int32, (sig_all, 128), 1), 8) < 4

        def put(i, slot):
            return pltpu.make_async_copy(
                held.at[slot], out_ref.at[pl.ds(i * step, step)], sems.at[slot]
            )

        def work(i, carry):
            slot = lax.rem(i, slots)

            @pl.when(i >= slots)
            def _():
                put(i - slots, slot).wait()

            for c in range(step):
                x = x_ref[i * step + c]
                turned = jnp.where(part, pltpu.roll(x, 124, 1), -pltpu.roll(x, 4, 1))
                x = x.astype(jnp.bfloat16)
                both = jnp.concatenate([x, turned.astype(jnp.bfloat16)], axis=0)
                value = lax.dot_general(both, x, NT_DIMS, preferred_element_type=jnp.float32)
                value = (value * scale).astype(jnp.bfloat16)
                held[slot, c, 0, 0] = value[:sig_all]
                held[slot, c, 0, 1] = value[sig_all:]
            put(i, slot).start()
            return carry

        lax.fori_loop(0, n_steps, work, 0)
        for i in range(n_steps - slots, n_steps):
            put(i, i % slots).wait()

    return pl.pallas_call(
        kernel,
        out_shape=jax.ShapeDtypeStruct((band_local, 1, 2, sig_all, sig_all), jnp.bfloat16),
        in_specs=[pl.BlockSpec(memory_space=pltpu.VMEM)],
        out_specs=pl.BlockSpec(memory_space=pl.ANY),
        scratch_shapes=[
            pltpu.VMEM((slots, step, 1, 2, sig_all, sig_all), jnp.bfloat16),
            pltpu.SemaphoreType.DMA((slots,)),
        ],
        compiler_params=pltpu.CompilerParams(vmem_limit_bytes=16 * 2**20),
        name="correlate",
    )


def per_device(samples, coarse_taps, fine_taps):
    n_win, n_sta = lax.axis_size("win"), lax.axis_size("sta")
    sig_local, samp_local = samples.shape
    tap_count, frame_len = coarse_taps.shape
    fine_tap_count, fine_len = fine_taps.shape
    frame_count = samp_local // frame_len
    band_local = KEEP // n_win
    frames = samples.reshape(sig_local, frame_count, frame_len)
    channelise = make_channeliser(
        n_win, n_sta, sig_local, frame_count, tap_count, frame_len, fine_tap_count, fine_len
    )
    fine = channelise(
        frames,
        coarse_taps,
        fine_taps,
        jnp.asarray(coarse_matrix(frame_len, KEEP)),
        jnp.asarray(fine_matrix(fine_len)),
        jnp.asarray(pick_matrix(band_local, 8, 128)),
    )
    frame_total = n_win * (frame_count // fine_len)
    correlate = make_correlator(band_local, n_sta * sig_local, 1.0 / frame_total)
    return correlate(fine.reshape(band_local, n_sta * sig_local, 128))


def solution(mesh):
    placed = (P("sta", "win"), P(), P())
    return jax.shard_map(
        per_device,
        mesh=mesh,
        in_specs=placed,
        out_specs=P("win", "sta", None, None, None),
        check_vma=False,
    )
```
